32 devices in a mesh: dp: 2 (over x), expert: 4 (over y, core), mp: 4 (over z).
Axes of the slice: x: 2, y: 2, z: 4, core: 2. Of those that a mesh axis runs over, the one named last changes fastest.
Arguments:
- tokens: bfloat16 [1024, 2048], P(('dp', 'expert'), 'mp'), parts along dimension 0, may hold values from -6 to 6
- routes: int32 [1024, 2], P(('dp', 'expert')), parts along dimension 0, may hold values from 0 to 3, all different within a row; in each aligned block of 128 rows (0 to 127, 128 to 255, ...) at most 96 rows name the same one
- gate_num: int32 [1024], P(('dp', 'expert')), parts along dimension 0, may hold values from 1 to 63
- capacity: int32 [4], replicated, may hold values from 48 to 96
- w_up: bfloat16 [2048, 28672], P(None, ('expert', 'mp')), may hold values from -0.125 to 0.125
- w_down: bfloat16 [28672, 2048], P(('expert', 'mp')), may hold values from -0.0625 to 0.0625
Outputs:
- mixed: bfloat16 [1024, 2048], P(('dp', 'expert'), 'mp'), parts along dimension 0
The draws below stay inside these ranges and needn't reach their ends.
There are 2 independent parts, one for each index of `dp`. The reference program is written for one: setup_inputs(seed, part) draws one part's arguments, and reference() takes and returns one part's arrays. A program takes and returns all parts, laid end to end along the dimension named above; an argument that names none is the same for every part. Nothing has to cross between parts.
Inputs may be any that keep to these rules, and one draw needn't show every extreme that they name: `routes`: each row names two different experts; in each aligned block of 128 rows no expert is named by more than 96 rows, a bound that some block reaches.
All inputs are finite; a program needn't handle non-finite values.
Results may differ from the reference program's by a relative error of at most 0.0085.
Values may be sent and summed in bfloat16 or wider, within the bound.
A program may use at most 64 MiB of HBM per device.

```python
import math
import jax
import jax.numpy as jnp
import numpy as np
from jax import lax

D = 2048
FF = 7168
TOK_DEV = 128
GROUP = 1
EXPERTS = 4
CAP = 96
TOKENS = 512
N_EXPERT = 4
N_MP = 4


def with_ends(drawn, own_key, smallest, largest):
    index_at = [jax.random.randint(jax.random.fold_in(own_key, axis), (), 0, length) for axis, length in enumerate(drawn.shape)]
    widest = drawn.shape.index(max(drawn.shape))
    neighbour = index_at[:widest] + [(index_at[widest] + 1) % drawn.shape[widest]] + index_at[widest + 1:]
    return drawn.at[tuple(index_at)].set(smallest).at[tuple(neighbour)].set(largest)


def block_levels(rng, dims, cuts, low, top_value):
    loudness = 1.0
    for axis_at, shards_of in cuts:
        draws = jax.random.uniform(jax.random.fold_in(jax.random.fold_in(rng, 6), axis_at), (shards_of,), jnp.float32, low / len(cuts), top_value / len(cuts))
        loudness = loudness * jnp.repeat(jnp.exp(draws), dims[axis_at] // shards_of).reshape((-1,) + (1,) * (len(dims) - 1 - axis_at))
    return loudness


def shared_out(key, own, number, rows, count, top, limit, lean):
    order = jax.random.permutation(key, count)
    heavy_load, ordinary = portions_of(count, rows * top, limit, lean, True), portions_of(count, rows * top, limit, lean, False)
    places = jnp.arange(count)

    def named(sizes, offset_by):
        used = int((sizes > 0).sum())
        fixed = max(1, used // 4)
        shifted = fixed + (places - fixed + offset_by * (used - fixed)) % max(1, count - fixed)
        return jnp.zeros((count,), jnp.int32).at[order[jnp.where(places < fixed, places, shifted)]].set(jnp.asarray(sizes, jnp.int32))

    sizes = jnp.where(number % 4 == 0, named(heavy_load, number // 4), named(ordinary, number - number // 4 - 1))
    mixed = jax.random.permutation(jax.random.fold_in(own, 3), count)
    donor, taker = mixed[0:count // 2 * 2:2], mixed[1:count // 2 * 2:2]
    margin = jnp.minimum(sizes[donor] - 1, limit - sizes[taker]) // 2
    margin = jnp.where((donor == order[0]) | (taker == order[0]) | (sizes[taker] == 0), 0, jnp.maximum(margin, 0))
    shifted = jax.random.randint(jax.random.fold_in(own, 4), (count // 2,), 0, 1 << 20) % (margin + 1)
    sizes = sizes.at[donor].add(-shifted).at[taker].add(shifted)
    labels = jnp.searchsorted(jnp.cumsum(sizes), jnp.arange(rows * top), side="right").astype(jnp.int32)
    listing = labels.reshape(top, rows).T
    listing = listing[jax.random.permutation(jax.random.fold_in(own, 1), rows)]
    offset_by = jax.random.randint(jax.random.fold_in(own, 2), (rows, 1), 0, top)
    return jnp.take_along_axis(listing, (jnp.arange(top)[None, :] + offset_by) % top, axis=1)


def portions_of(number_of, total, bound, lean, full):
    loads = [(1 << 20) // math.isqrt(rank ** lean) + 1 for rank in range(1, number_of + 1)]
    largest = bound if full else min(bound, max(-(-total // number_of), total * loads[0] // sum(loads)))
    least = 1 if total - largest >= number_of - 1 else 0
    given, surplus = [largest] + [least] * (number_of - 1), total - largest - least * (number_of - 1)
    while surplus > 0:
        candidates = [i for i in range(1, number_of) if given[i] < largest] or [i for i in range(1, number_of) if given[i] < bound]
        mass, remaining = sum([loads[i] for i in candidates]), surplus
        for i in candidates:
            addition = min(bound - given[i], max(1, remaining * loads[i] // mass), surplus)
            given[i] = given[i] + addition
            surplus = surplus - addition
    return np.array(given)


def normal_values(key, shape, scale, limit, shards=(), held_as=jnp.bfloat16):
    array = jax.random.normal(key, shape, jnp.float32) * scale
    if len(shards) > 0:
        array = block_levels(key, shape, shards, -0.22, 0.18) * array
    return jnp.clip(array, min=-limit, max=limit).astype(held_as)


def setup_inputs(seed: int = 0, part: int = 0) -> dict:
    arg_keys = jax.random.split(jax.random.key(seed), 7)
    part_keys = jax.random.split(jax.random.fold_in(arg_keys[6], part), 7)
    tokens = normal_values(part_keys[0], (TOKENS, D), 1.0, 6.0, ((0, 4), (1, 4)))
    routes_keys = jax.random.split(jax.random.fold_in(part_keys[1], 1), TOKENS // TOK_DEV)
    routes_turns = jax.random.permutation(jax.random.fold_in(part_keys[1], 3), TOKENS // TOK_DEV)
    routes = jax.vmap(lambda own, number: shared_out(jax.random.fold_in(part_keys[1], 2), own, number, TOK_DEV, EXPERTS, 2, CAP, 2))(routes_keys, routes_turns).reshape((TOKENS, 2))
    gate_num = with_ends(jax.random.randint(part_keys[2], (TOKENS,), 1, 64), jax.random.fold_in(part_keys[2], 1), 1, 63).astype(jnp.int32)
    capacity = with_ends(jax.random.randint(arg_keys[3], (EXPERTS,), CAP // 2, CAP + 1), jax.random.fold_in(arg_keys[3], 1), CAP // 2, CAP).astype(jnp.int32)
    w_up = normal_values(arg_keys[4], (D, EXPERTS * FF), D ** -0.5, 0.125, ((1, 16),))
    w_down = normal_values(arg_keys[5], (EXPERTS * FF, D), FF ** -0.5, 0.0625, ((0, 16),))
    return {"tokens": tokens, "routes": routes, "gate_num": gate_num, "capacity": capacity, "w_up": w_up, "w_down": w_down}


def reference(tokens, routes, gate_num, capacity, w_up, w_down):
    shard_count = GROUP * N_MP
    shard_width = FF // shard_count
    row_count = N_EXPERT * CAP
    expert_ids = jnp.arange(EXPERTS, dtype=jnp.int32)
    named_count = (routes[:, :, None] == expert_ids[None, None, :]).astype(jnp.int32).sum(axis=1)
    blocked = named_count.reshape(N_EXPERT, TOK_DEV, EXPERTS)
    positions = (jnp.cumsum(blocked, axis=1) - blocked).reshape(TOKENS, EXPERTS)
    route_pos = jnp.take_along_axis(positions, routes, axis=1)
    kept_mask = route_pos < capacity[routes]
    first_share = gate_num.astype(jnp.float32) / 64.0
    weights = jnp.stack([first_share, 1.0 - first_share], axis=1)
    source_block = jnp.arange(TOKENS, dtype=jnp.int32) // TOK_DEV
    slot_index = source_block[:, None] * CAP + route_pos
    token_ids = jnp.arange(2 * TOKENS, dtype=jnp.int32) // 2
    token_copies = tokens[token_ids]

    def per_expert(expert):
        chosen = (routes == expert) & kept_mask
        target = jnp.where(chosen, slot_index, row_count).reshape(-1).astype(jnp.int32)
        slot_rows = jnp.zeros((row_count + 1, D), jnp.bfloat16).at[target].set(token_copies)[:row_count]
        up_cols = lax.dynamic_slice_in_dim(w_up, expert * FF, FF, 1)
        hidden = jax.nn.silu(jnp.dot(slot_rows, up_cols, preferred_element_type=jnp.float32)).astype(jnp.bfloat16)
        down_rows = lax.dynamic_slice_in_dim(w_down, expert * FF, FF, 0)

        def add_shard(running, shard_id):
            hidden_part = lax.dynamic_slice_in_dim(hidden, shard_id * shard_width, shard_width, 1)
            down_part = lax.dynamic_slice_in_dim(down_rows, shard_id * shard_width, shard_width, 0)
            partial_value = jnp.dot(hidden_part, down_part, preferred_element_type=jnp.float32).astype(jnp.bfloat16)
            partial_value = lax.optimization_barrier(partial_value)
            return running + partial_value.astype(jnp.float32), None

        start = jnp.zeros((row_count, D), jnp.float32)
        return lax.scan(add_shard, start, jnp.arange(shard_count, dtype=jnp.int32))[0]

    expert_out = lax.map(per_expert, expert_ids)
    flat_index = (routes * row_count + jnp.where(kept_mask, slot_index, 0)).astype(jnp.int32)
    values = expert_out.reshape(EXPERTS * row_count, D)[flat_index]
    scaled = jnp.where(kept_mask, weights, 0.0)
    mixed = jnp.sum(scaled[:, :, None] * values, axis=1)
    return mixed.astype(jnp.bfloat16)
```

```python
import functools

import jax
import jax.numpy as jnp
from jax import lax
from jax.experimental import pallas as pl
from jax.experimental.pallas import tpu as pltpu
from jax.sharding import PartitionSpec as P


def per_device_collectives(tokens, routes, gate_num, capacity, w_up, w_down):
    token_count = routes.shape[0]
    expert_count = capacity.shape[0]
    group_size = lax.axis_size("expert") // expert_count
    slot_count = min(token_count, 3 * token_count // expert_count)
    feature_width = w_up.shape[0]
    expert_ids = jnp.arange(expert_count, dtype=jnp.int32)
    matches = routes[:, :, None] == expert_ids[None, None, :]
    named_count = matches.sum(axis=1).astype(jnp.float32)
    token_ids = jnp.arange(token_count, dtype=jnp.int32)
    lower_mask = (token_ids[:, None] > token_ids[None, :]).astype(jnp.float32)
    positions = jnp.dot(
        lower_mask, named_count, precision=lax.Precision.HIGHEST, preferred_element_type=jnp.float32
    ).astype(jnp.int32)
    route_pos = jnp.sum(jnp.where(matches, positions[:, None, :], 0), axis=2)
    route_cap = jnp.sum(jnp.where(matches, capacity[None, None, :], 0), axis=2)
    kept_mask = route_pos < route_cap
    slot_index = jnp.where(kept_mask, routes * slot_count + route_pos, -1)
    first_share = gate_num.astype(jnp.float32) / 64.0
    weights = jnp.where(kept_mask, jnp.stack([first_share, 1.0 - first_share], axis=1), 0.0)
    slot_ids = jnp.arange(expert_count * slot_count, dtype=jnp.int32)
    dispatch_matrix = jnp.any(slot_ids[:, None, None] == slot_index[None, :, :], axis=2).astype(
        jnp.bfloat16
    )
    combine_hits = slot_ids[None, :, None] == slot_index[:, None, :]
    combine_matrix = jnp.sum(jnp.where(combine_hits, weights[:, None, :], 0.0), axis=2)
    whole = lax.all_gather(tokens, "mp", axis=1, tiled=True)
    buffer = jnp.dot(dispatch_matrix, whole, preferred_element_type=jnp.float32).astype(
        jnp.bfloat16
    )
    width = buffer.shape[1]
    grouped = buffer.reshape(expert_count, 1, slot_count, width)
    copies = jnp.broadcast_to(grouped, (expert_count, group_size, slot_count, width))
    received = lax.all_to_all(
        copies.reshape(expert_count * group_size, slot_count, width),
        "expert",
        split_axis=0,
        concat_axis=0,
        tiled=True,
    )
    source_count, count_here, width = received.shape
    flat_rows = received.reshape(source_count * count_here, width)
    hidden = jax.nn.silu(jnp.dot(flat_rows, w_up, preferred_element_type=jnp.float32)).astype(
        jnp.bfloat16
    )
    partial_value = jnp.dot(hidden, w_down, preferred_element_type=jnp.float32).astype(jnp.bfloat16)
    answered = lax.all_to_all(
        partial_value.reshape(source_count, count_here, width),
        "expert",
        split_axis=0,
        concat_axis=0,
        tiled=True,
    )
    summed = (
        answered.astype(jnp.float32)
        .reshape(expert_count, group_size, slot_count, feature_width)
        .sum(axis=1)
    )
    summed = summed.reshape(expert_count * slot_count, feature_width)
    mixed = jnp.dot(
        combine_matrix, summed, precision=lax.Precision.HIGHEST, preferred_element_type=jnp.float32
    )
    return lax.psum_scatter(mixed, "mp", scatter_dimension=1, tiled=True).astype(jnp.bfloat16)

MESH = pl.DeviceIdType.MESH


def flip(index, bits):
    result, place = 0, 1
    while place <= bits:
        bit = lax.rem(index // place, 2)
        result = result + place * (lax.rem(bit + 1, 2) if bits & place else bit)
        place *= 2
    return result + index // place * place


def expert_kernel(
    pieces,
    slot_count,
    tile,
    tokens_ref,
    meta_ref,
    capacity_ref,
    w_up_ref,
    w_down_ref,
    out_ref,
    up_buf,
    down_buf,
    rows_buf,
    meta_buf,
    slots_buf,
    pick_buf,
    mix_buf,
    acc_buf,
    hidden_buf,
    core_out,
    core_in,
    keep_buf,
    y_out,
    y_in,
    z_out,
    z_in,
    up_sem,
    down_sem,
    meta_send,
    meta_recv,
    zs,
    zr,
    ys,
    yr,
    cs,
    cr,
    core_send,
    core_recv,
    ysum_send,
    ysum_recv,
    zsum_send,
    zsum_recv,
):
    token_count, piece_width = tokens_ref.shape
    hidden_width = up_buf.shape[1]
    e = lax.axis_index("expert")
    m = lax.axis_index("mp")
    partner = {"expert": flip(e, 1)}
    across = {"expert": flip(e, 2)}
    peers = [None] + [{"mp": flip(m, j)} for j in range(1, pieces)]

    up_copies, down_copies = [], []
    for j in range(pieces):
        start = pl.multiple_of(flip(m, j) * piece_width, piece_width)
        up_copies.append(
            pltpu.make_async_copy(
                w_up_ref.at[pl.ds(start, piece_width), :], up_buf.at[pl.ds(j * piece_width, piece_width), :], up_sem.at[j]
            )
        )
    for copy in up_copies:
        copy.start()
    down_copy = pltpu.make_async_copy(w_down_ref, down_buf, down_sem)
    down_copy.start()

    barrier = pltpu.get_barrier_semaphore()
    for device in [partner, across] + peers[1:]:
        pl.semaphore_signal(barrier, inc=1, device_id=device, device_id_type=MESH)
    pl.semaphore_wait(barrier, pieces + 1)

    def send(src, dst, send_sem, recv_sem, device):
        copy = pltpu.make_async_remote_copy(
            src_ref=src, dst_ref=dst, send_sem=send_sem, recv_sem=recv_sem, device_id=device, device_id_type=MESH
        )
        return copy

    meta_copies = [
        send(meta_ref, meta_buf.at[1], meta_send.at[0], meta_recv.at[0], partner),
        send(meta_ref, meta_buf.at[2], meta_send.at[1], meta_recv.at[1], across),
        send(meta_buf.at[2], meta_buf.at[3], meta_send.at[2], meta_recv.at[2], partner),
    ]
    z_copies = [None] + [
        send(tokens_ref, rows_buf.at[0, j], zs.at[j], zr.at[j], peers[j]) for j in range(1, pieces)
    ]

    def own(j):
        return tokens_ref if j == 0 else rows_buf.at[0, j]

    y_copies = [send(own(j), rows_buf.at[2, j], ys.at[j], yr.at[j], across) for j in range(pieces)]
    c_copies = [send(own(j), rows_buf.at[1, j], cs.at[0, j], cr.at[0, j], partner) for j in range(pieces)]
    d_copies = [
        send(rows_buf.at[2, j], rows_buf.at[3, j], cs.at[1, j], cr.at[1, j], partner) for j in range(pieces)
    ]
    meta_copies[0].start()
    meta_copies[1].start()
    for j in range(1, pieces):
        z_copies[j].start()
    y_copies[0].start()
    c_copies[0].start()

    def from_z(j):
        z_copies[j].wait_recv()
        y_copies[j].start()
        c_copies[j].start()

    def from_y(j):
        y_copies[j].wait_recv()
        d_copies[j].start()

    def select():
        meta_copies[0].wait_recv()
        meta_copies[2].wait_recv()
        limit = capacity_ref[e].astype(jnp.float32)
        before = lax.broadcasted_iota(jnp.int32, (token_count, token_count), 0)
        after = lax.broadcasted_iota(jnp.int32, (token_count, token_count), 1)
        earlier = jnp.where(before < after, 1.0, 0.0).astype(jnp.bfloat16)
        slot_ids = lax.broadcasted_iota(jnp.int32, (slot_count, token_count), 0).astype(jnp.float32)
        for r in range(4):
            meta = meta_ref[...] if r == 0 else meta_buf[r]
            first, second, gate = meta[0:1, :], meta[1:2, :], meta[2:3, :]
            named = jnp.where((first == e) | (second == e), 1.0, 0.0)
            position = jnp.dot(
                jnp.broadcast_to(named, (16, token_count)).astype(jnp.bfloat16),
                earlier,
                preferred_element_type=jnp.float32,
            )[0:1, :]
            slot = jnp.where((named > 0.5) & (position < limit), position, -1.0)
            share = gate.astype(jnp.float32) / 64.0
            weight = jnp.where(first == e, share, 1.0 - share)
            hit = jnp.where(slot_ids == slot, 1.0, 0.0)
            pick_buf[r] = hit.astype(jnp.bfloat16)
            mix_buf[r] = (hit * weight).astype(jnp.bfloat16)

    def up_piece(j):
        c_copies[j].wait_recv()
        d_copies[j].wait_recv()
        up_copies[j].wait()
        for r in range(4):
            rows = own(j)[...] if r == 0 else rows_buf[r, j]
            slots_buf[pl.ds(r * slot_count, slot_count), :] = jnp.dot(
                pick_buf[r], rows, preferred_element_type=jnp.float32
            ).astype(jnp.bfloat16)

        def column(i, carry):
            columns = pl.ds(pl.multiple_of(i * tile, tile), tile)
            value = jnp.dot(
                slots_buf[...],
                up_buf[pl.ds(j * piece_width, piece_width), columns],
                preferred_element_type=jnp.float32,
            )
            if j > 0:
                value = acc_buf[:, columns] + value
            if j < pieces - 1:
                acc_buf[:, columns] = value
            else:
                hidden_buf[:, columns] = (value / (1.0 + jnp.exp(-value))).astype(jnp.bfloat16)
            return carry

        lax.fori_loop(0, hidden_width // tile, column, 0)

    meta_copies[1].wait_recv()
    meta_copies[2].start()
    select()
    if pieces > 1:
        from_z(1)
    from_y(0)
    for j in range(pieces):
        up_piece(j)
        if j + 2 < pieces:
            from_z(j + 2)
        if j + 1 < pieces:
            from_y(j + 1)

    down_copy.wait()
    core_copies = [
        send(core_out.at[j], core_in.at[j], core_send.at[j], core_recv.at[j], partner) for j in range(pieces)
    ]
    ysum_copies = [send(y_out.at[j], y_in.at[j], ysum_send.at[j], ysum_recv.at[j], across) for j in range(pieces)]
    zsum_copies = [None] + [
        send(z_out.at[j], z_in.at[j], zsum_send.at[j], zsum_recv.at[j], peers[j]) for j in range(1, pieces)
    ]

    def down_piece(j):
        base = flip(m, j) * piece_width

        def column(i, carry):
            local = pl.ds(pl.multiple_of(i * tile, tile), tile)
            columns = pl.ds(pl.multiple_of(base + i * tile, tile), tile)
            partial = jnp.dot(
                hidden_buf[...], down_buf[:, columns], preferred_element_type=jnp.float32
            ).astype(jnp.bfloat16)
            for r in (1, 3, 0, 2):
                mixed = lax.dot_general(
                    mix_buf[r],
                    partial[r * slot_count : (r + 1) * slot_count, :],
                    (((0,), (0,)), ((), ())),
                    preferred_element_type=jnp.float32,
                )
                if r % 2 == 1:
                    core_out[j, r // 2, :, local] = mixed.astype(jnp.bfloat16)
                else:
                    keep_buf[j, r // 2, :, local] = mixed
            return carry

        lax.fori_loop(0, piece_width // tile, column, 0)
        core_copies[j].start()

    def to_y(j):
        core_copies[j].wait_recv()
        y_out[j] = (keep_buf[j, 1] + core_in[j, 1].astype(jnp.float32)).astype(jnp.bfloat16)
        ysum_copies[j].start()

    def own_sum(j):
        ysum_copies[j].wait_recv()
        return keep_buf[j, 0] + core_in[j, 0].astype(jnp.float32) + y_in[j].astype(jnp.float32)

    def to_z(j):
        z_out[j] = own_sum(j).astype(jnp.bfloat16)
        zsum_copies[j].start()

    order = list(range(pieces - 1, -1, -1))
    for step in range(pieces + 2):
        if step < pieces:
            down_piece(order[step])
        if 1 <= step <= pieces:
            to_y(order[step - 1])
        if step >= 2 and order[step - 2] > 0:
            to_z(order[step - 2])
    total = own_sum(0)
    for j in range(pieces - 1, 0, -1):
        zsum_copies[j].wait_recv()
        total = total + z_in[j].astype(jnp.float32)
    out_ref[...] = total.astype(jnp.bfloat16)
    for copy in (
        meta_copies + z_copies[1:] + y_copies + c_copies + d_copies + core_copies + ysum_copies + zsum_copies[1:]
    ):
        copy.wait_send()


def per_device_kernel(tokens, routes, gate_num, capacity, w_up, w_down):
    token_count, piece_width = tokens.shape
    pieces = lax.axis_size("mp")
    expert_count = capacity.shape[0]
    slot_count = min(token_count, 3 * token_count // expert_count)
    width, hidden_width = w_up.shape
    row_count = expert_count * slot_count
    tile = min(256, piece_width)
    meta = jnp.concatenate(
        [routes.T, gate_num[None, :], jnp.zeros((5, token_count), jnp.int32)], axis=0
    )
    bf16, f32 = jnp.bfloat16, jnp.float32
    sem = pltpu.SemaphoreType.DMA
    block = (token_count, piece_width)
    return pl.pallas_call(
        functools.partial(expert_kernel, pieces, slot_count, tile),
        out_shape=jax.ShapeDtypeStruct(block, bf16),
        in_specs=[
            pl.BlockSpec(memory_space=pltpu.VMEM),
            pl.BlockSpec(memory_space=pltpu.VMEM),
            pl.BlockSpec(memory_space=pltpu.SMEM),
            pl.BlockSpec(memory_space=pl.ANY),
            pl.BlockSpec(memory_space=pl.ANY),
        ],
        out_specs=pl.BlockSpec(memory_space=pltpu.VMEM),
        scratch_shapes=[
            pltpu.VMEM((width, hidden_width), bf16),
            pltpu.VMEM((hidden_width, width), bf16),
            pltpu.VMEM((4, pieces) + block, bf16),
            pltpu.VMEM((4, 8, token_count), jnp.int32),
            pltpu.VMEM((row_count, piece_width), bf16),
            pltpu.VMEM((4, slot_count, token_count), bf16),
            pltpu.VMEM((4, slot_count, token_count), bf16),
            pltpu.VMEM((row_count, hidden_width), f32),
            pltpu.VMEM((row_count, hidden_width), bf16),
            pltpu.VMEM((pieces, 2) + block, bf16),
            pltpu.VMEM((pieces, 2) + block, bf16),
            pltpu.VMEM((pieces, 2) + block, f32),
            pltpu.VMEM((pieces,) + block, bf16),
            pltpu.VMEM((pieces,) + block, bf16),
            pltpu.VMEM((pieces,) + block, bf16),
            pltpu.VMEM((pieces,) + block, bf16),
            sem((pieces,)),
            sem,
            sem((3,)),
            sem((3,)),
            sem((pieces,)),
            sem((pieces,)),
            sem((pieces,)),
            sem((pieces,)),
            sem((2, pieces)),
            sem((2, pieces)),
            sem((pieces,)),
            sem((pieces,)),
            sem((pieces,)),
            sem((pieces,)),
            sem((pieces,)),
            sem((pieces,)),
        ],
        compiler_params=pltpu.CompilerParams(collective_id=0, has_side_effects=True),
    )(tokens, meta, capacity, w_up, w_down)


def per_device(tokens, routes, gate_num, capacity, w_up, w_down):
    experts, pieces = lax.axis_size("expert"), lax.axis_size("mp")
    weight_bytes = 2 * w_up.size * w_up.dtype.itemsize
    fits = experts == 4 and capacity.shape[0] == 4 and pieces & (pieces - 1) == 0
    fits = fits and weight_bytes <= 24 << 20 and tokens.shape[0] == 128
    fits = fits and tokens.shape[1] % 256 == 0 and w_up.shape[1] % 256 == 0
    body = per_device_kernel if fits else per_device_collectives
    return body(tokens, routes, gate_num, capacity, w_up, w_down)


def solution(mesh):
    return jax.shard_map(
        per_device,
        mesh=mesh,
        in_specs=(
            P(("dp", "expert"), "mp"),
            P(("dp", "expert"), None),
            P(("dp", "expert")),
            P(),
            P(None, ("expert", "mp")),
            P(("expert", "mp"), None),
        ),
        out_specs=P(("dp", "expert"), "mp"),
        check_vma=False,
    )
```

```python
import functools

import jax
import jax.numpy as jnp
from jax import lax
from jax.experimental import pallas as pl
from jax.experimental.pallas import tpu as pltpu
from jax.sharding import PartitionSpec as P


def per_device_collectives(tokens, routes, gate_num, capacity, w_up, w_down):
    token_count = routes.shape[0]
    expert_count = capacity.shape[0]
    group_size = lax.axis_size("expert") // expert_count
    slot_count = min(token_count, 3 * token_count // expert_count)
    feature_width = w_up.shape[0]
    expert_ids = jnp.arange(expert_count, dtype=jnp.int32)
    matches = routes[:, :, None] == expert_ids[None, None, :]
    named_count = matches.sum(axis=1).astype(jnp.float32)
    token_ids = jnp.arange(token_count, dtype=jnp.int32)
    lower_mask = (token_ids[:, None] > token_ids[None, :]).astype(jnp.float32)
    positions = jnp.dot(
        lower_mask, named_count, precision=lax.Precision.HIGHEST, preferred_element_type=jnp.float32
    ).astype(jnp.int32)
    route_pos = jnp.sum(jnp.where(matches, positions[:, None, :], 0), axis=2)
    route_cap = jnp.sum(jnp.where(matches, capacity[None, None, :], 0), axis=2)
    kept_mask = route_pos < route_cap
    slot_index = jnp.where(kept_mask, routes * slot_count + route_pos, -1)
    first_share = gate_num.astype(jnp.float32) / 64.0
    weights = jnp.where(kept_mask, jnp.stack([first_share, 1.0 - first_share], axis=1), 0.0)
    slot_ids = jnp.arange(expert_count * slot_count, dtype=jnp.int32)
    dispatch_matrix = jnp.any(slot_ids[:, None, None] == slot_index[None, :, :], axis=2).astype(
        jnp.bfloat16
    )
    combine_hits = slot_ids[None, :, None] == slot_index[:, None, :]
    combine_matrix = jnp.sum(jnp.where(combine_hits, weights[:, None, :], 0.0), axis=2)
    whole = lax.all_gather(tokens, "mp", axis=1, tiled=True)
    buffer = jnp.dot(dispatch_matrix, whole, preferred_element_type=jnp.float32).astype(
        jnp.bfloat16
    )
    width = buffer.shape[1]
    grouped = buffer.reshape(expert_count, 1, slot_count, width)
    copies = jnp.broadcast_to(grouped, (expert_count, group_size, slot_count, width))
    received = lax.all_to_all(
        copies.reshape(expert_count * group_size, slot_count, width),
        "expert",
        split_axis=0,
        concat_axis=0,
        tiled=True,
    )
    source_count, count_here, width = received.shape
    flat_rows = received.reshape(source_count * count_here, width)
    hidden = jax.nn.silu(jnp.dot(flat_rows, w_up, preferred_element_type=jnp.float32)).astype(
        jnp.bfloat16
    )
    partial_value = jnp.dot(hidden, w_down, preferred_element_type=jnp.float32).astype(jnp.bfloat16)
    answered = lax.all_to_all(
        partial_value.reshape(source_count, count_here, width),
        "expert",
        split_axis=0,
        concat_axis=0,
        tiled=True,
    )
    summed = (
        answered.astype(jnp.float32)
        .reshape(expert_count, group_size, slot_count, feature_width)
        .sum(axis=1)
    )
    summed = summed.reshape(expert_count * slot_count, feature_width)
    mixed = jnp.dot(
        combine_matrix, summed, precision=lax.Precision.HIGHEST, preferred_element_type=jnp.float32
    )
    return lax.psum_scatter(mixed, "mp", scatter_dimension=1, tiled=True).astype(jnp.bfloat16)

MESH = pl.DeviceIdType.MESH
SLOTS = 4


def expert_kernel(
    slot_count,
    tile,
    tokens_ref,
    routes_ref,
    gate_ref,
    capacity_ref,
    w_up_ref,
    w_down_ref,
    out_ref,
    up_buf,
    down_buf,
    rows_buf,
    routes_buf,
    gate_buf,
    slots_buf,
    pick_buf,
    mix_buf,
    acc_buf,
    hidden_buf,
    core_out,
    core_in,
    keep_buf,
    y_out,
    y_in,
    z_out,
    z_in,
    up_sem,
    down_sem,
    meta_send,
    meta_recv,
    zs,
    zr,
    ys,
    yr,
    cs,
    cr,
    core_send,
    core_recv,
    ysum_send,
    ysum_recv,
    zsum_send,
    zsum_recv,
):
    token_count, piece_width = tokens_ref.shape
    hidden_width = up_buf.shape[1]
    half_rows, half_cols = token_count // 2, piece_width // 2
    f32, bf16 = jnp.float32, jnp.bfloat16
    e = lax.axis_index("expert")
    m = lax.axis_index("mp")
    upper = m // 2
    inner = lax.rem(lax.rem(m, 2) + upper, 2)
    pair_index = m + 1 - 2 * lax.rem(m, 2)
    facing_index = 3 - m
    piece_of = [m, pair_index, 2 - upper, 3 - 3 * upper]
    partner = {"expert": e + 1 - 2 * lax.rem(e, 2)}
    across = {"expert": lax.rem(e + 2, 4)}
    pair, facing = {"mp": pair_index}, {"mp": facing_index}
    onward = {"mp": inner * facing_index + (1 - inner) * pair_index}
    is_inner, is_end = inner == 1, inner == 0
    halves = range(2)

    up_copies = []
    for s in range(SLOTS):
        start = pl.multiple_of(piece_of[s] * piece_width, piece_width)
        up_copies.append(
            pltpu.make_async_copy(
                w_up_ref.at[pl.ds(start, piece_width), :],
                up_buf.at[pl.ds(s * piece_width, piece_width), :],
                up_sem.at[s],
            )
        )
    for copy in up_copies:
        copy.start()
    down_copy = pltpu.make_async_copy(w_down_ref, down_buf, down_sem)
    down_copy.start()

    barrier = pltpu.get_barrier_semaphore()
    for device in (partner, across, pair):
        pl.semaphore_signal(barrier, inc=1, device_id=device, device_id_type=MESH)

    @pl.when(is_inner)
    def _():
        pl.semaphore_signal(barrier, inc=1, device_id=facing, device_id_type=MESH)

    pl.semaphore_wait(barrier, 3 + inner)

    def send(src, dst, send_sem, recv_sem, device):
        return pltpu.make_async_remote_copy(
            src_ref=src, dst_ref=dst, send_sem=send_sem, recv_sem=recv_sem, device_id=device, device_id_type=MESH
        )

    def own(s, h):
        rows = pl.ds(h * half_rows, half_rows)
        return tokens_ref.at[rows, :] if s == 0 else rows_buf.at[0, s, rows, :]

    def slot(r, s, h):
        return rows_buf.at[r, s, pl.ds(h * half_rows, half_rows), :]

    meta_copies = []
    for i, (ref, buf) in enumerate(((routes_ref, routes_buf), (gate_ref, gate_buf))):
        meta_copies.append(
            (
                send(ref, buf.at[1], meta_send.at[i, 0], meta_recv.at[i, 0], partner),
                send(ref, buf.at[2], meta_send.at[i, 1], meta_recv.at[i, 1], across),
                send(buf.at[2], buf.at[3], meta_send.at[i, 2], meta_recv.at[i, 2], partner),
            )
        )
    to_pair = [send(own(0, h), slot(0, 1, h), zs.at[0, h], zr.at[1, h], pair) for h in halves]
    relays = {}
    relays[0] = [send(own(0, h), slot(0, 2, h), zs.at[1, h], zr.at[2, h], facing) for h in halves]
    relays[1] = [send(slot(0, 1, h), slot(0, 3, h), zs.at[2, h], zr.at[3, h], facing) for h in halves]
    relays[2] = [send(slot(0, 2, h), slot(0, 2, h), zs.at[3, h], zr.at[2, h], pair) for h in halves]
    relays[3] = [send(slot(0, 3, h), slot(0, 3, h), zs.at[4, h], zr.at[3, h], pair) for h in halves]
    z_arrivals = {1: to_pair, 2: relays[0], 3: relays[1]}

    y_copies = [[send(own(s, h), slot(2, s, h), ys.at[s, h], yr.at[s, h], across) for h in halves] for s in range(SLOTS)]
    c_copies = [
        [send(own(s, h), slot(1, s, h), cs.at[0, s, h], cr.at[0, s, h], partner) for h in halves] for s in range(SLOTS)
    ]
    d_copies = [
        [send(slot(2, s, h), slot(3, s, h), cs.at[1, s, h], cr.at[1, s, h], partner) for h in halves]
        for s in range(SLOTS)
    ]

    def spread(s, h):
        if s > 0:
            z_arrivals[s][h].wait_recv()

        @pl.when(is_inner)
        def _():
            relays[s][h].start()

        y_copies[s][h].start()
        c_copies[s][h].start()

    def from_y(s, h):
        y_copies[s][h].wait_recv()
        d_copies[s][h].start()

    def select():
        for copies in meta_copies:
            copies[0].wait_recv()
            copies[2].wait_recv()
        limit = capacity_ref[e].astype(f32)
        before = lax.broadcasted_iota(jnp.int32, (token_count, token_count), 0)
        after = lax.broadcasted_iota(jnp.int32, (token_count, token_count), 1)
        earlier = jnp.where(before < after, 1.0, 0.0).astype(bf16)
        slot_ids = lax.broadcasted_iota(jnp.int32, (slot_count, token_count), 0).astype(f32)
        for r in range(4):
            routes = routes_ref[...] if r == 0 else routes_buf[r]
            gate = gate_ref[...] if r == 0 else gate_buf[r]
            first, second = routes[0:1, :], routes[1:2, :]
            named = jnp.where((first == e) | (second == e), 1.0, 0.0)
            position = jnp.dot(
                jnp.broadcast_to(named, (16, token_count)).astype(bf16), earlier, preferred_element_type=f32
            )[0:1, :]
            place = jnp.where((named > 0.5) & (position < limit), position, -1.0)
            share = gate.astype(f32) / 64.0
            weight = jnp.where(first == e, share, 1.0 - share)
            hit = jnp.where(slot_ids == place, 1.0, 0.0)
            pick_buf[r] = hit.astype(bf16)
            mix_buf[r] = (hit * weight).astype(bf16)

    def up_piece(s):
        for h in halves:
            c_copies[s][h].wait_recv()
            d_copies[s][h].wait_recv()
        up_copies[s].wait()
        for r in range(4):
            rows = tokens_ref[...] if r == 0 and s == 0 else rows_buf[r, s]
            slots_buf[pl.ds(r * slot_count, slot_count), :] = jnp.dot(
                pick_buf[r], rows, preferred_element_type=f32
            ).astype(bf16)

        def column(i, carry):
            columns = pl.ds(pl.multiple_of(i * tile, tile), tile)
            value = jnp.dot(
                slots_buf[...], up_buf[pl.ds(s * piece_width, piece_width), columns], preferred_element_type=f32
            )
            if s > 0:
                value = acc_buf[:, columns] + value
            if s < SLOTS - 1:
                acc_buf[:, columns] = value
            else:
                hidden_buf[:, columns] = (value / (1.0 + jnp.exp(-value))).astype(bf16)
            return carry

        lax.fori_loop(0, hidden_width // tile, column, 0)

    for copies in meta_copies:
        copies[0].start()
        copies[1].start()
    for h in halves:
        to_pair[h].start()
        spread(0, h)
    for copies in meta_copies:
        copies[1].wait_recv()
        copies[2].start()
    select()
    for h in halves:
        spread(1, h)
        from_y(0, h)
    for h in halves:
        spread(2, h)

    @pl.when(is_inner)
    def _():
        for h in halves:
            z_arrivals[3][h].wait_recv()
            relays[3][h].start()
            y_copies[3][h].start()
            c_copies[3][h].start()

    up_piece(0)

    @pl.when(is_end)
    def _():
        for h in halves:
            z_arrivals[3][h].wait_recv()
            y_copies[3][h].start()
            c_copies[3][h].start()

    for h in halves:
        from_y(1, h)
    up_piece(1)
    for h in halves:
        from_y(2, h)
    from_y(3, 0)
    up_piece(2)
    from_y(3, 1)
    up_piece(3)

    down_copy.wait()

    core_copies = [
        [send(core_out.at[s, h], core_in.at[s, h], core_send.at[s, h], core_recv.at[s, h], partner) for h in halves]
        for s in range(SLOTS)
    ]
    ysum_copies = [
        [send(y_out.at[s, h], y_in.at[s, h], ysum_send.at[s, h], ysum_recv.at[s, h], across) for h in halves]
        for s in range(SLOTS)
    ]
    zsum_copies = {}
    for s in (1, 2, 3):
        place, device = (2, pair) if s == 1 else (3 - s + 3 * inner, onward)
        zsum_copies[s] = [
            send(z_out.at[s, h], z_in.at[place, h], zsum_send.at[s, h], zsum_recv.at[place, h], device) for h in halves
        ]

    def z_arrived(place, h):
        send(z_out.at[1, h], z_in.at[place, h], zsum_send.at[1, h], zsum_recv.at[place, h], pair).wait_recv()
        return z_in[place, h].astype(f32)

    def down_piece(s, h):
        columns = pl.ds(pl.multiple_of(piece_of[s] * piece_width + h * half_cols, half_cols), half_cols)
        partial = jnp.dot(hidden_buf[...], down_buf[:, columns], preferred_element_type=f32).astype(bf16)
        for r in (1, 3, 0, 2):
            mixed = lax.dot_general(
                mix_buf[r],
                partial[r * slot_count : (r + 1) * slot_count, :],
                (((0,), (0,)), ((), ())),
                preferred_element_type=f32,
            )
            if r % 2 == 1:
                core_out[s, h, r // 2] = mixed.astype(bf16)
            else:
                keep_buf[s, h, r // 2] = mixed
        core_copies[s][h].start()

    def to_y(s, h):
        core_copies[s][h].wait_recv()
        y_out[s, h] = (keep_buf[s, h, 1] + core_in[s, h, 1].astype(f32)).astype(bf16)
        ysum_copies[s][h].start()

    def own_sum(s, h):
        ysum_copies[s][h].wait_recv()
        return keep_buf[s, h, 0] + core_in[s, h, 0].astype(f32) + y_in[s, h].astype(f32)

    def end_to_z(s, h):
        @pl.when(is_end)
        def _():
            z_out[s, h] = own_sum(s, h).astype(bf16)
            zsum_copies[s][h].start()

    def inner_to_z(s, h):
        @pl.when(is_inner)
        def _():
            place = 3 if s == 1 else 3 - s
            z_out[s, h] = (own_sum(s, h) + z_arrived(place, h)).astype(bf16)
            zsum_copies[s][h].start()

    order = [(s, h) for s in (3, 2, 1, 0) for h in halves]
    for step in range(len(order) + 1):
        if step < len(order):
            down_piece(*order[step])
        if step >= 1:
            to_y(*order[step - 1])
        if 5 <= step < 9:
            end_to_z(*order[step - 5])
    for step in range(4):
        inner_to_z(*order[step])
    for h in halves:
        end_to_z(1, h)
    for h in halves:
        inner_to_z(1, h)
    for h in halves:
        total = own_sum(0, h) + z_arrived(2, h)
        keep_buf[0, h, 0] = total

        @pl.when(is_inner)
        def _():
            keep_buf[0, h, 0] = keep_buf[0, h, 0] + z_arrived(4, h)

        out_ref[:, h * half_cols : (h + 1) * half_cols] = keep_buf[0, h, 0].astype(bf16)

    for copies in meta_copies:
        for copy in copies:
            copy.wait_send()
    for h in halves:
        to_pair[h].wait_send()
        for s in range(SLOTS):
            y_copies[s][h].wait_send()
            c_copies[s][h].wait_send()
            d_copies[s][h].wait_send()
            core_copies[s][h].wait_send()
            ysum_copies[s][h].wait_send()
            if s > 0:
                zsum_copies[s][h].wait_send()

    @pl.when(is_inner)
    def _():
        for s in range(SLOTS):
            for h in halves:
                relays[s][h].wait_send()


def per_device_kernel(tokens, routes, gate_num, capacity, w_up, w_down):
    token_count, piece_width = tokens.shape
    expert_count = capacity.shape[0]
    slot_count = min(token_count, 3 * token_count // expert_count)
    width, hidden_width = w_up.shape
    row_count = expert_count * slot_count
    bf16, f32 = jnp.bfloat16, jnp.float32
    sem = pltpu.SemaphoreType.DMA
    block = (token_count, piece_width)
    half = (token_count, piece_width // 2)
    in_vmem = pl.BlockSpec(memory_space=pltpu.VMEM)
    return pl.pallas_call(
        functools.partial(expert_kernel, slot_count, 256),
        out_shape=jax.ShapeDtypeStruct(block, bf16),
        in_specs=[in_vmem] * 3
        + [pl.BlockSpec(memory_space=pltpu.SMEM)]
        + [pl.BlockSpec(memory_space=pl.ANY)] * 2,
        out_specs=in_vmem,
        scratch_shapes=[
            pltpu.VMEM((width, hidden_width), bf16),
            pltpu.VMEM((hidden_width, width), bf16),
            pltpu.VMEM((4, SLOTS) + block, bf16),
            pltpu.VMEM((4, 2, token_count), jnp.int32),
            pltpu.VMEM((4, 1, token_count), jnp.int32),
            pltpu.VMEM((row_count, piece_width), bf16),
            pltpu.VMEM((4, slot_count, token_count), bf16),
            pltpu.VMEM((4, slot_count, token_count), bf16),
            pltpu.VMEM((row_count, hidden_width), f32),
            pltpu.VMEM((row_count, hidden_width), bf16),
            pltpu.VMEM((SLOTS, 2, 2) + half, bf16),
            pltpu.VMEM((SLOTS, 2, 2) + half, bf16),
            pltpu.VMEM((SLOTS, 2, 2) + half, f32),
            pltpu.VMEM((SLOTS, 2) + half, bf16),
            pltpu.VMEM((SLOTS, 2) + half, bf16),
            pltpu.VMEM((SLOTS, 2) + half, bf16),
            pltpu.VMEM((5, 2) + half, bf16),
            sem((SLOTS,)),
            sem,
            sem((2, 3)),
            sem((2, 3)),
            sem((5, 2)),
            sem((SLOTS, 2)),
            sem((SLOTS, 2)),
            sem((SLOTS, 2)),
            sem((2, SLOTS, 2)),
            sem((2, SLOTS, 2)),
            sem((SLOTS, 2)),
            sem((SLOTS, 2)),
            sem((SLOTS, 2)),
            sem((SLOTS, 2)),
            sem((SLOTS, 2)),
            sem((5, 2)),
        ],
        compiler_params=pltpu.CompilerParams(
            collective_id=0, has_side_effects=True, vmem_limit_bytes=58 << 20
        ),
    )(tokens, routes.T, gate_num[None, :], capacity, w_up, w_down)


def per_device(tokens, routes, gate_num, capacity, w_up, w_down):
    experts, pieces = lax.axis_size("expert"), lax.axis_size("mp")
    weight_bytes = 2 * w_up.size * w_up.dtype.itemsize
    fits = experts == 4 and capacity.shape[0] == 4 and pieces == SLOTS
    fits = fits and weight_bytes <= 24 << 20 and tokens.shape[0] == 128
    fits = fits and tokens.shape[1] % 256 == 0 and w_up.shape[1] % 256 == 0
    body = per_device_kernel if fits else per_device_collectives
    return body(tokens, routes, gate_num, capacity, w_up, w_down)


def solution(mesh):
    return jax.shard_map(
        per_device,
        mesh=mesh,
        in_specs=(
            P(("dp", "expert"), "mp"),
            P(("dp", "expert"), None),
            P(("dp", "expert")),
            P(),
            P(None, ("expert", "mp")),
            P(("expert", "mp"), None),
        ),
        out_specs=P(("dp", "expert"), "mp"),
        check_vma=False,
    )
```

```python
import functools

import jax
import jax.numpy as jnp
from jax import lax
from jax.experimental import pallas as pl
from jax.experimental.pallas import tpu as pltpu
from jax.sharding import PartitionSpec as P


def per_device_collectives(tokens, routes, gate_num, capacity, w_up, w_down):
    token_count = routes.shape[0]
    expert_count = capacity.shape[0]
    group_size = lax.axis_size("expert") // expert_count
    slot_count = min(token_count, 3 * token_count // expert_count)
    feature_width = w_up.shape[0]
    expert_ids = jnp.arange(expert_count, dtype=jnp.int32)
    matches = routes[:, :, None] == expert_ids[None, None, :]
    named_count = matches.sum(axis=1).astype(jnp.float32)
    token_ids = jnp.arange(token_count, dtype=jnp.int32)
    lower_mask = (token_ids[:, None] > token_ids[None, :]).astype(jnp.float32)
    positions = jnp.dot(
        lower_mask, named_count, precision=lax.Precision.HIGHEST, preferred_element_type=jnp.float32
    ).astype(jnp.int32)
    route_pos = jnp.sum(jnp.where(matches, positions[:, None, :], 0), axis=2)
    route_cap = jnp.sum(jnp.where(matches, capacity[None, None, :], 0), axis=2)
    kept_mask = route_pos < route_cap
    slot_index = jnp.where(kept_mask, routes * slot_count + route_pos, -1)
    first_share = gate_num.astype(jnp.float32) / 64.0
    weights = jnp.where(kept_mask, jnp.stack([first_share, 1.0 - first_share], axis=1), 0.0)
    slot_ids = jnp.arange(expert_count * slot_count, dtype=jnp.int32)
    dispatch_matrix = jnp.any(slot_ids[:, None, None] == slot_index[None, :, :], axis=2).astype(
        jnp.bfloat16
    )
    combine_hits = slot_ids[None, :, None] == slot_index[:, None, :]
    combine_matrix = jnp.sum(jnp.where(combine_hits, weights[:, None, :], 0.0), axis=2)
    whole = lax.all_gather(tokens, "mp", axis=1, tiled=True)
    buffer = jnp.dot(dispatch_matrix, whole, preferred_element_type=jnp.float32).astype(
        jnp.bfloat16
    )
    width = buffer.shape[1]
    grouped = buffer.reshape(expert_count, 1, slot_count, width)
    copies = jnp.broadcast_to(grouped, (expert_count, group_size, slot_count, width))
    received = lax.all_to_all(
        copies.reshape(expert_count * group_size, slot_count, width),
        "expert",
        split_axis=0,
        concat_axis=0,
        tiled=True,
    )
    source_count, count_here, width = received.shape
    flat_rows = received.reshape(source_count * count_here, width)
    hidden = jax.nn.silu(jnp.dot(flat_rows, w_up, preferred_element_type=jnp.float32)).astype(
        jnp.bfloat16
    )
    partial_value = jnp.dot(hidden, w_down, preferred_element_type=jnp.float32).astype(jnp.bfloat16)
    answered = lax.all_to_all(
        partial_value.reshape(source_count, count_here, width),
        "expert",
        split_axis=0,
        concat_axis=0,
        tiled=True,
    )
    summed = (
        answered.astype(jnp.float32)
        .reshape(expert_count, group_size, slot_count, feature_width)
        .sum(axis=1)
    )
    summed = summed.reshape(expert_count * slot_count, feature_width)
    mixed = jnp.dot(
        combine_matrix, summed, precision=lax.Precision.HIGHEST, preferred_element_type=jnp.float32
    )
    return lax.psum_scatter(mixed, "mp", scatter_dimension=1, tiled=True).astype(jnp.bfloat16)

MESH = pl.DeviceIdType.MESH
SLOTS = 4


def expert_kernel(
    slot_count,
    tile,
    tokens_ref,
    routes_ref,
    gate_ref,
    capacity_ref,
    w_up_ref,
    w_down_ref,
    out_ref,
    up_buf,
    down_buf,
    rows_buf,
    routes_buf,
    gate_buf,
    slots_buf,
    pick_buf,
    mix_buf,
    acc_buf,
    hidden_buf,
    core_out,
    core_in,
    keep_buf,
    y_out,
    y_in,
    z_out,
    z_in,
    own_sem,
    up_sem,
    down_sem,
    meta_send,
    meta_recv,
    zs,
    zr,
    ys,
    yr,
    cs,
    cr,
    core_send,
    core_recv,
    ysum_send,
    ysum_recv,
    zsum_send,
    zsum_recv,
):
    token_count, piece_width = tokens_ref.shape
    hidden_width = up_buf.shape[1]
    half_rows, half_cols = token_count // 2, piece_width // 2
    f32, bf16 = jnp.float32, jnp.bfloat16
    e = lax.axis_index("expert")
    m = lax.axis_index("mp")
    upper = m // 2
    inner = lax.rem(lax.rem(m, 2) + upper, 2)
    pair_index = m + 1 - 2 * lax.rem(m, 2)
    facing_index = 3 - m
    piece_of = [m, pair_index, 2 - upper, 3 - 3 * upper]
    partner = {"expert": e + 1 - 2 * lax.rem(e, 2)}
    across = {"expert": lax.rem(e + 2, 4)}
    pair, facing = {"mp": pair_index}, {"mp": facing_index}
    onward = {"mp": inner * facing_index + (1 - inner) * pair_index}
    is_inner, is_end = inner == 1, inner == 0
    halves = range(2)

    own_copies = [
        pltpu.make_async_copy(tokens_ref, rows_buf.at[0, 0], own_sem.at[0]),
        pltpu.make_async_copy(routes_ref, routes_buf.at[0], own_sem.at[1]),
        pltpu.make_async_copy(gate_ref, gate_buf.at[0], own_sem.at[2]),
    ]
    for copy in own_copies:
        copy.start()
    up_copies = []
    for s in range(SLOTS):
        start = pl.multiple_of(piece_of[s] * piece_width, piece_width)
        up_copies.append(
            pltpu.make_async_copy(
                w_up_ref.at[pl.ds(start, piece_width), :],
                up_buf.at[pl.ds(s * piece_width, piece_width), :],
                up_sem.at[s],
            )
        )
    barrier = pltpu.get_barrier_semaphore()
    for device in (partner, across, pair):
        pl.semaphore_signal(barrier, inc=1, device_id=device, device_id_type=MESH)

    @pl.when(is_inner)
    def _():
        pl.semaphore_signal(barrier, inc=1, device_id=facing, device_id_type=MESH)

    for copy in up_copies:
        copy.start()
    down_copy = pltpu.make_async_copy(w_down_ref, down_buf, down_sem)
    down_copy.start()
    for copy in own_copies:
        copy.wait()
    pl.semaphore_wait(barrier, 3 + inner)

    def send(src, dst, send_sem, recv_sem, device):
        return pltpu.make_async_remote_copy(
            src_ref=src, dst_ref=dst, send_sem=send_sem, recv_sem=recv_sem, device_id=device, device_id_type=MESH
        )

    def slot(r, s, h):
        return rows_buf.at[r, s, pl.ds(h * half_rows, half_rows), :]

    meta_copies = []
    for i, buf in enumerate((routes_buf, gate_buf)):
        meta_copies.append(
            (
                send(buf.at[0], buf.at[1], meta_send.at[i, 0], meta_recv.at[i, 0], partner),
                send(buf.at[0], buf.at[2], meta_send.at[i, 1], meta_recv.at[i, 1], across),
                send(buf.at[2], buf.at[3], meta_send.at[i, 2], meta_recv.at[i, 2], partner),
            )
        )
    to_pair = [send(slot(0, 0, h), slot(0, 1, h), zs.at[0, h], zr.at[1, h], pair) for h in halves]
    relays = {}
    relays[0] = [send(slot(0, 0, h), slot(0, 2, h), zs.at[1, h], zr.at[2, h], facing) for h in halves]
    relays[1] = [send(slot(0, 1, h), slot(0, 3, h), zs.at[2, h], zr.at[3, h], facing) for h in halves]
    relays[2] = [send(slot(0, 2, h), slot(0, 2, h), zs.at[3, h], zr.at[2, h], pair) for h in halves]
    relays[3] = [send(slot(0, 3, h), slot(0, 3, h), zs.at[4, h], zr.at[3, h], pair) for h in halves]
    z_arrivals = {1: to_pair, 2: relays[0], 3: relays[1]}

    y_copies = [[send(slot(0, s, h), slot(2, s, h), ys.at[s, h], yr.at[s, h], across) for h in halves] for s in range(SLOTS)]
    c_copies = [
        [send(slot(0, s, h), slot(1, s, h), cs.at[0, s, h], cr.at[0, s, h], partner) for h in halves] for s in range(SLOTS)
    ]
    d_copies = [
        [send(slot(2, s, h), slot(3, s, h), cs.at[1, s, h], cr.at[1, s, h], partner) for h in halves]
        for s in range(SLOTS)
    ]

    def spread(s, h, relay):
        if s > 0:
            z_arrivals[s][h].wait_recv()
        if relay:
            relays[s][h].start()
        y_copies[s][h].start()
        c_copies[s][h].start()

    def by_role(inner_step, end_step):
        @pl.when(is_inner)
        def _():
            for s, h in inner_step:
                spread(s, h, True)

        @pl.when(is_end)
        def _():
            for s, h in end_step:
                spread(s, h, False)

    def from_y(s, h):
        y_copies[s][h].wait_recv()
        d_copies[s][h].start()

    def select():
        for copies in meta_copies:
            copies[0].wait_recv()
            copies[2].wait_recv()
        limit = capacity_ref[e].astype(f32)
        before = lax.broadcasted_iota(jnp.int32, (token_count, token_count), 0)
        after = lax.broadcasted_iota(jnp.int32, (token_count, token_count), 1)
        earlier = jnp.where(before < after, 1.0, 0.0).astype(bf16)
        slot_ids = lax.broadcasted_iota(jnp.int32, (slot_count, token_count), 0).astype(f32)
        for r in range(4):
            routes = routes_buf[r]
            gate = gate_buf[r]
            first, second = routes[0:1, :], routes[1:2, :]
            named = jnp.where((first == e) | (second == e), 1.0, 0.0)
            position = jnp.dot(
                jnp.broadcast_to(named, (16, token_count)).astype(bf16), earlier, preferred_element_type=f32
            )[0:1, :]
            place = jnp.where((named > 0.5) & (position < limit), position, -1.0)
            share = gate.astype(f32) / 64.0
            weight = jnp.where(first == e, share, 1.0 - share)
            hit = jnp.where(slot_ids == place, 1.0, 0.0)
            pick_buf[r] = hit.astype(bf16)
            mix_buf[r] = (hit * weight).astype(bf16)

    def up_rows(s):
        for r in range(4):
            for h in halves:
                if r == 1:
                    c_copies[s][h].wait_recv()
                if r == 3:
                    d_copies[s][h].wait_recv()
            slots_buf[pl.ds(r * slot_count, slot_count), :] = jnp.dot(
                pick_buf[r], rows_buf[r, s], preferred_element_type=f32
            ).astype(bf16)
        up_copies[s].wait()

    def up_columns(s, start, end):
        def column(i, carry):
            columns = pl.ds(pl.multiple_of(i * tile, tile), tile)
            value = jnp.dot(
                slots_buf[...], up_buf[pl.ds(s * piece_width, piece_width), columns], preferred_element_type=f32
            )
            if s > 0:
                value = acc_buf[:, columns] + value
            if s < SLOTS - 1:
                acc_buf[:, columns] = value
            else:
                hidden_buf[:, columns] = (value / (1.0 + jnp.exp(-value))).astype(bf16)
            return carry

        lax.fori_loop(start, end, column, 0)

    tiles = hidden_width // tile
    third, half_way = tiles // 3, tiles // 2
    for h in halves:
        to_pair[h].start()
        by_role([(0, h)], [(0, h)])
    for copies in meta_copies:
        copies[0].start()
        copies[1].start()
    for copies in meta_copies:
        copies[1].wait_recv()
        copies[2].start()
    select()
    for h in halves:
        by_role([(1, h), (2, h)], [(1, h)])
        from_y(0, h)
    up_rows(0)
    up_columns(0, 0, third)
    by_role([(3, 0)], [(2, 0)])
    up_columns(0, third, 2 * third)
    by_role([(3, 1)], [(2, 1)])
    from_y(1, 0)
    from_y(1, 1)
    up_columns(0, 2 * third, tiles)
    up_rows(1)
    up_columns(1, 0, half_way)
    by_role([], [(3, 0)])
    up_columns(1, half_way, tiles)
    by_role([], [(3, 1)])
    from_y(2, 0)
    from_y(2, 1)
    up_rows(2)
    up_columns(2, 0, half_way)
    from_y(3, 0)
    up_columns(2, half_way, tiles)
    from_y(3, 1)
    up_rows(3)
    up_columns(3, 0, tiles)

    down_copy.wait()

    core_copies = [
        [send(core_out.at[s, h], core_in.at[s, h], core_send.at[s, h], core_recv.at[s, h], partner) for h in halves]
        for s in range(SLOTS)
    ]
    ysum_copies = [
        [send(y_out.at[s, h], y_in.at[s, h], ysum_send.at[s, h], ysum_recv.at[s, h], across) for h in halves]
        for s in range(SLOTS)
    ]
    zsum_copies = {}
    for s in (1, 2, 3):
        place, device = (2, pair) if s == 1 else (3 - s + 3 * inner, onward)
        zsum_copies[s] = [
            send(z_out.at[s, h], z_in.at[place, h], zsum_send.at[s, h], zsum_recv.at[place, h], device) for h in halves
        ]

    def z_arrived(place, h):
        send(z_out.at[1, h], z_in.at[place, h], zsum_send.at[1, h], zsum_recv.at[place, h], pair).wait_recv()
        return z_in[place, h].astype(f32)

    def down_piece(s, h):
        columns = pl.ds(pl.multiple_of(piece_of[s] * piece_width + h * half_cols, half_cols), half_cols)
        partial = jnp.dot(hidden_buf[...], down_buf[:, columns], preferred_element_type=f32).astype(bf16)
        for r in (1, 3, 0, 2):
            mixed = lax.dot_general(
                mix_buf[r],
                partial[r * slot_count : (r + 1) * slot_count, :],
                (((0,), (0,)), ((), ())),
                preferred_element_type=f32,
            )
            if r % 2 == 1:
                core_out[s, h, r // 2] = mixed.astype(bf16)
            else:
                keep_buf[s, h, r // 2] = mixed
        core_copies[s][h].start()

    def to_y(s, h):
        core_copies[s][h].wait_recv()
        y_out[s, h] = (keep_buf[s, h, 1] + core_in[s, h, 1].astype(f32)).astype(bf16)
        ysum_copies[s][h].start()

    def own_sum(s, h):
        ysum_copies[s][h].wait_recv()
        return keep_buf[s, h, 0] + core_in[s, h, 0].astype(f32) + y_in[s, h].astype(f32)

    def end_to_z(s, h):
        @pl.when(is_end)
        def _():
            z_out[s, h] = own_sum(s, h).astype(bf16)
            zsum_copies[s][h].start()

    def inner_to_z(s, h):
        @pl.when(is_inner)
        def _():
            place = 3 if s == 1 else 3 - s
            z_out[s, h] = (own_sum(s, h) + z_arrived(place, h)).astype(bf16)
            zsum_copies[s][h].start()

    order = [(s, h) for s in (3, 2, 1, 0) for h in halves]
    for step in range(len(order) + 1):
        if step < len(order):
            down_piece(*order[step])
        if step >= 1:
            to_y(*order[step - 1])
        if 4 <= step < 8:
            end_to_z(*order[step - 4])
        if step >= 7:
            inner_to_z(*order[step - 7])
    for step in (2, 3):
        inner_to_z(*order[step])
    for h in halves:
        end_to_z(1, h)
    for h in halves:
        inner_to_z(1, h)
    for h in halves:
        total = own_sum(0, h) + z_arrived(2, h)
        keep_buf[0, h, 0] = total

        @pl.when(is_inner)
        def _():
            keep_buf[0, h, 0] = keep_buf[0, h, 0] + z_arrived(4, h)

        out_ref[:, h * half_cols : (h + 1) * half_cols] = keep_buf[0, h, 0].astype(bf16)

    for copies in meta_copies:
        for copy in copies:
            copy.wait_send()
    for h in halves:
        to_pair[h].wait_send()
        for s in range(SLOTS):
            y_copies[s][h].wait_send()
            c_copies[s][h].wait_send()
            d_copies[s][h].wait_send()
            core_copies[s][h].wait_send()
            ysum_copies[s][h].wait_send()
            if s > 0:
                zsum_copies[s][h].wait_send()

    @pl.when(is_inner)
    def _():
        for s in range(SLOTS):
            for h in halves:
                relays[s][h].wait_send()


def per_device_kernel(tokens, routes, gate_num, capacity, w_up, w_down):
    token_count, piece_width = tokens.shape
    expert_count = capacity.shape[0]
    slot_count = min(token_count, 3 * token_count // expert_count)
    width, hidden_width = w_up.shape
    row_count = expert_count * slot_count
    bf16, f32 = jnp.bfloat16, jnp.float32
    sem = pltpu.SemaphoreType.DMA
    block = (token_count, piece_width)
    half = (token_count, piece_width // 2)
    in_vmem, in_hbm = pl.BlockSpec(memory_space=pltpu.VMEM), pl.BlockSpec(memory_space=pltpu.HBM)
    return pl.pallas_call(
        functools.partial(expert_kernel, slot_count, 256),
        out_shape=jax.ShapeDtypeStruct(block, bf16),
        in_specs=[in_hbm] * 3 + [pl.BlockSpec(memory_space=pltpu.SMEM)] + [in_hbm] * 2,
        out_specs=in_vmem,
        scratch_shapes=[
            pltpu.VMEM((width, hidden_width), bf16),
            pltpu.VMEM((hidden_width, width), bf16),
            pltpu.VMEM((4, SLOTS) + block, bf16),
            pltpu.VMEM((4, 2, token_count), jnp.int32),
            pltpu.VMEM((4, 1, token_count), jnp.int32),
            pltpu.VMEM((row_count, piece_width), bf16),
            pltpu.VMEM((4, slot_count, token_count), bf16),
            pltpu.VMEM((4, slot_count, token_count), bf16),
            pltpu.VMEM((row_count, hidden_width), f32),
            pltpu.VMEM((row_count, hidden_width), bf16),
            pltpu.VMEM((SLOTS, 2, 2) + half, bf16),
            pltpu.VMEM((SLOTS, 2, 2) + half, bf16),
            pltpu.VMEM((SLOTS, 2, 2) + half, f32),
            pltpu.VMEM((SLOTS, 2) + half, bf16),
            pltpu.VMEM((SLOTS, 2) + half, bf16),
            pltpu.VMEM((SLOTS, 2) + half, bf16),
            pltpu.VMEM((5, 2) + half, bf16),
            sem((3,)),
            sem((SLOTS,)),
            sem,
            sem((2, 3)),
            sem((2, 3)),
            sem((5, 2)),
            sem((SLOTS, 2)),
            sem((SLOTS, 2)),
            sem((SLOTS, 2)),
            sem((2, SLOTS, 2)),
            sem((2, SLOTS, 2)),
            sem((SLOTS, 2)),
            sem((SLOTS, 2)),
            sem((SLOTS, 2)),
            sem((SLOTS, 2)),
            sem((SLOTS, 2)),
            sem((5, 2)),
        ],
        compiler_params=pltpu.CompilerParams(
            collective_id=0, has_side_effects=True, vmem_limit_bytes=58 << 20
        ),
    )(tokens, routes.T, gate_num[None, :], capacity, w_up, w_down)


def per_device(tokens, routes, gate_num, capacity, w_up, w_down):
    experts, pieces = lax.axis_size("expert"), lax.axis_size("mp")
    weight_bytes = 2 * w_up.size * w_up.dtype.itemsize
    fits = experts == 4 and capacity.shape[0] == 4 and pieces == SLOTS
    fits = fits and weight_bytes <= 24 << 20 and tokens.shape[0] == 128
    fits = fits and tokens.shape[1] % 256 == 0 and w_up.shape[1] % 256 == 0
    body = per_device_kernel if fits else per_device_collectives
    return body(tokens, routes, gate_num, capacity, w_up, w_down)


def solution(mesh):
    return jax.shard_map(
        per_device,
        mesh=mesh,
        in_specs=(
            P(("dp", "expert"), "mp"),
            P(("dp", "expert"), None),
            P(("dp", "expert")),
            P(),
            P(None, ("expert", "mp")),
            P(("expert", "mp"), None),
        ),
        out_specs=P(("dp", "expert"), "mp"),
        check_vma=False,
    )
```
